32 devices in a mesh: section: 4 (over y, core), expert: 8 (over z, x).
Axes of the slice: x: 2, y: 2, z: 4, core: 2. Of those that a mesh axis runs over, the one named last changes fastest.
Arguments:
- pending_inputs: bfloat16 [4, 256, 4096], P('section', 'expert'), may hold values from -6 to 6
- arriving_microgroups: bfloat16 [1, 256, 4096], P(None, 'expert'), may hold values from -6 to 6
- expert_assignment: int32 [4, 2, 256, 2], P('section', None, 'expert'), may hold values from 0 to 3, all different within a row; in each aligned block of 32 rows (0 to 31, 32 to 63, ..., all dimensions but the last counted through in order) at most 24 rows name the same one
- segment_rescale_factor: float32 [4, 4096], P('section'), may hold values from 0.5 to 1.5
- assignment_logit_maps: float32 [4, 4096, 4], P('section'), may hold values from -0.09375 to 0.09375
- gating_projections: bfloat16 [4, 4096, 28672], P('section', None, 'expert'), may hold values from -0.09375 to 0.09375
- expanding_projections: bfloat16 [4, 4096, 28672], P('section', None, 'expert'), may hold values from -0.09375 to 0.09375
- contracting_projections: bfloat16 [4, 28672, 4096], P('section', 'expert'), may hold values from -0.0625 to 0.0625
Outputs:
- carried: bfloat16 [2, 4, 256, 4096], P(None, 'section', 'expert')
The draws below stay inside these ranges and needn't reach their ends.
Inputs may be any that keep to these rules, and one draw needn't show every extreme that they name: `expert_assignment`: the two experts of a row differ. Among the rows of one device (one section, one step, 32 tokens), no expert is named more than 24 times, and in every draw some expert is named exactly 24 times.
All inputs are finite; a program needn't handle non-finite values.
Results may differ from the reference program's by a relative error of at most 0.0085.
Values may be sent and summed in bfloat16 or wider, within the bound.
No kernel may reach another device: no remote copies, remote signals or barrier semaphores. Data moves between devices by JAX's collectives and lax.ppermute only.
A program may use at most 128 MiB of HBM per device.

```python
import math
import jax
import jax.numpy as jnp
import numpy as np
from jax import lax

HIDDEN_WIDTH = 4096
FF = 7168
EXPERTS = 4
STEPS = 2
TOK_DEV = 32
CAP = 24
MICRO_SEQ_COUNT = 256
N_SECTION = 4
N_EXPERT = 8


def level_of(rng, dims, cuts, smallest, largest):
    def one(axis_at, shards_of):
        steps = jax.random.uniform(jax.random.fold_in(jax.random.fold_in(rng, 6), axis_at), (shards_of,), jnp.float32, smallest / len(cuts), largest / len(cuts))
        return jnp.repeat(jnp.exp(steps), dims[axis_at] // shards_of).reshape((-1,) + (1,) * (len(dims) - axis_at - 1))

    loudness = one(*cuts[0])
    for cut in cuts[1:]:
        loudness = loudness * one(*cut)
    return loudness


def deal_out(rng, own, number, rows, count, top, most, lean):
    ranking = jax.random.permutation(rng, count)
    crowded, usual = portions_of(count, rows * top, most, lean, True), portions_of(count, rows * top, most, lean, False)
    places = jnp.arange(count)

    def named(sizes, rotation):
        used = int((sizes > 0).sum())
        fixed = max(1, used // 4)
        shifted = fixed + (places - fixed + rotation * (used - fixed)) % max(1, count - fixed)
        return jnp.zeros((count,), jnp.int32).at[ranking[jnp.where(places < fixed, places, shifted)]].set(jnp.asarray(sizes, jnp.int32))

    sizes = jnp.where(number % 4 == 0, named(crowded, number // 4), named(usual, number - number // 4 - 1))
    mixed = jax.random.permutation(jax.random.fold_in(own, 3), count)
    source_of, taker = mixed[0:count // 2 * 2:2], mixed[1:count // 2 * 2:2]
    room = jnp.minimum(sizes[source_of] - 1, most - sizes[taker]) // 2
    room = jnp.where((source_of == ranking[0]) | (taker == ranking[0]) | (sizes[taker] == 0), 0, jnp.maximum(room, 0))
    shifted = jax.random.randint(jax.random.fold_in(own, 4), (count // 2,), 0, 1 << 20) % (room + 1)
    sizes = sizes.at[source_of].add(-shifted).at[taker].add(shifted)
    items = jnp.searchsorted(jnp.cumsum(sizes), jnp.arange(rows * top), side="right").astype(jnp.int32)
    listing = items.reshape(top, rows).T
    listing = listing[jax.random.permutation(jax.random.fold_in(own, 1), rows)]
    rotation = jax.random.randint(jax.random.fold_in(own, 2), (rows, 1), 0, top)
    return jnp.take_along_axis(listing, (jnp.arange(top)[None, :] + rotation) % top, axis=1)


def portions_of(number_of, total, most, skew, full):
    loads = [(1 << 20) // math.isqrt(rank ** skew) + 1 for rank in range(1, number_of + 1)]
    largest = most if full else min(most, max(-(-total // number_of), total * loads[0] // sum(loads)))
    least = 1 if total - largest >= number_of - 1 else 0
    counts, surplus = [largest] + [least] * (number_of - 1), total - largest - least * (number_of - 1)
    while surplus > 0:
        candidates = [i for i in range(1, number_of) if counts[i] < largest] or [i for i in range(1, number_of) if counts[i] < most]
        pool, budget = sum([loads[i] for i in candidates]), surplus
        for i in candidates:
            addition = min(most - counts[i], max(1, budget * loads[i] // pool), surplus)
            counts[i] = counts[i] + addition
            surplus = surplus - addition
    return np.array(counts)


def scatter_about(key, shape, width, bound, pieces=(), kind=jnp.bfloat16):
    entries = width * jax.random.normal(key, shape, jnp.float32)
    if pieces:
        entries = entries * level_of(key, shape, pieces, -0.22, 0.18)
    return jnp.clip(entries, -bound, bound).astype(kind)


def setup_inputs(seed: int = 0) -> dict:
    splits = jax.random.split(jax.random.key(seed), 9)
    pending_inputs = scatter_about(splits[0], (N_SECTION, MICRO_SEQ_COUNT, HIDDEN_WIDTH), 1.0, 6.0, ((0, 4), (1, 8)))
    arriving_microgroups = scatter_about(splits[1], (STEPS - 1, MICRO_SEQ_COUNT, HIDDEN_WIDTH), 1.0, 6.0, ((1, 8),))
    expert_assignment_keys = jax.random.split(jax.random.fold_in(splits[2], 1), N_SECTION * STEPS * MICRO_SEQ_COUNT // TOK_DEV)
    expert_assignment_turns = jax.random.permutation(jax.random.fold_in(splits[2], 3), N_SECTION * STEPS * MICRO_SEQ_COUNT // TOK_DEV)
    expert_assignment = jax.vmap(lambda own, number: deal_out(jax.random.fold_in(splits[2], 2), own, number, TOK_DEV, EXPERTS, 2, CAP, 2))(expert_assignment_keys, expert_assignment_turns).reshape((N_SECTION, STEPS, MICRO_SEQ_COUNT, 2))
    segment_rescale_factor = jnp.clip(0.5 + 1.0 * jax.random.uniform(splits[3], (N_SECTION, HIDDEN_WIDTH), jnp.float32) ** level_of(splits[3], (N_SECTION, HIDDEN_WIDTH), ((0, 4),), -0.2, 0.2), 0.5, 1.5)
    assignment_logit_maps = scatter_about(splits[4], (N_SECTION, HIDDEN_WIDTH, EXPERTS), HIDDEN_WIDTH ** -0.5, 0.09375, ((0, 4),), jnp.float32)
    gating_projections = scatter_about(splits[5], (N_SECTION, HIDDEN_WIDTH, EXPERTS * FF), HIDDEN_WIDTH ** -0.5, 0.09375, ((0, 4), (2, 8)))
    expanding_projections = scatter_about(splits[6], (N_SECTION, HIDDEN_WIDTH, EXPERTS * FF), HIDDEN_WIDTH ** -0.5, 0.09375, ((0, 4), (2, 8)))
    contracting_projections = scatter_about(splits[7], (N_SECTION, EXPERTS * FF, HIDDEN_WIDTH), FF ** -0.5, 0.0625, ((0, 4), (1, 8)))
    return {"pending_inputs": pending_inputs, "arriving_microgroups": arriving_microgroups, "expert_assignment": expert_assignment, "segment_rescale_factor": segment_rescale_factor, "assignment_logit_maps": assignment_logit_maps, "gating_projections": gating_projections, "expanding_projections": expanding_projections, "contracting_projections": contracting_projections}


epsilon = 1e-05

def section_layer(activation, chosen, segment_rescale_factor, assignment_logit_maps, gating_projections, expanding_projections, contracting_projections):
    as_float = activation.astype(jnp.float32)
    normed = (as_float * lax.rsqrt(lax.optimization_barrier(jnp.mean(as_float * as_float, -1, keepdims=True)) + epsilon) * segment_rescale_factor).astype(jnp.bfloat16)
    logits = jnp.dot(normed.astype(jnp.float32), assignment_logit_maps, precision=lax.Precision.HIGHEST)
    chooses = chosen[:, :, None] == jnp.arange(EXPERTS, dtype=jnp.int32)[None, None, :]
    picked = lax.optimization_barrier(jnp.sum(jnp.where(chooses, logits[:, None, :], jnp.float32(0.0)), -1))
    first_share = jax.nn.sigmoid(picked[:, 0] - picked[:, 1])
    shares = jnp.stack([first_share, 1.0 - first_share], 1).astype(jnp.bfloat16).astype(jnp.float32).reshape(-1)
    chosen_flat = chosen.reshape(-1).astype(jnp.int32)
    token_owner = (jnp.arange(2 * MICRO_SEQ_COUNT, dtype=jnp.int32) // 2).astype(jnp.int32)
    capacity = N_EXPERT * CAP

    def one_expert(expert_id):
        matches = chosen_flat == expert_id
        index_list = jnp.nonzero(matches, size=capacity, fill_value=0)[0].astype(jnp.int32)
        live = jnp.arange(capacity, dtype=jnp.int32) < jnp.sum(matches.astype(jnp.int32))
        owners = token_owner[index_list]
        token_rows = normed[owners]
        gate_cols = lax.dynamic_slice_in_dim(gating_projections, (expert_id * FF).astype(jnp.int32), FF, 1)
        up_cols = lax.dynamic_slice_in_dim(expanding_projections, (expert_id * FF).astype(jnp.int32), FF, 1)
        down_rows = lax.dynamic_slice_in_dim(contracting_projections, (expert_id * FF).astype(jnp.int32), FF, 0)
        gate_value = jnp.dot(token_rows, gate_cols, preferred_element_type=jnp.float32)
        up_value = jnp.dot(token_rows, up_cols, preferred_element_type=jnp.float32)
        hidden = (jax.nn.silu(gate_value) * up_value).astype(jnp.bfloat16)
        output = jnp.dot(hidden, down_rows, preferred_element_type=jnp.float32)
        weight = jnp.where(live, shares[index_list], jnp.float32(0.0))
        return jnp.zeros((MICRO_SEQ_COUNT, HIDDEN_WIDTH), jnp.float32).at[owners].add(output * weight[:, None])
    mixture = lax.optimization_barrier(jnp.sum(lax.map(one_expert, jnp.arange(EXPERTS, dtype=jnp.int32)), 0))
    return (as_float + mixture).astype(jnp.bfloat16)

def reference(pending_inputs, arriving_microgroups, expert_assignment, segment_rescale_factor, assignment_logit_maps, gating_projections, expanding_projections, contracting_projections):
    activation_sequence = [pending_inputs[segment_ordinal] for segment_ordinal in range(N_SECTION)]
    records = []
    for step_index in range(STEPS):
        if step_index > 0:
            activation_sequence[0] = arriving_microgroups[step_index - 1]
        results = [section_layer(activation_sequence[segment_ordinal], expert_assignment[segment_ordinal, step_index], segment_rescale_factor[segment_ordinal], assignment_logit_maps[segment_ordinal], gating_projections[segment_ordinal], expanding_projections[segment_ordinal], contracting_projections[segment_ordinal]) for segment_ordinal in range(N_SECTION)]
        activation_sequence = [results[(segment_ordinal - 1) % N_SECTION] for segment_ordinal in range(N_SECTION)]
        records.append(jnp.stack(activation_sequence))
    return jnp.stack(records)
```

```python
import jax
import jax.numpy as jnp
from jax import lax
from jax.experimental import pallas as pl
from jax.experimental.pallas import tpu as pltpu
from jax.sharding import PartitionSpec as P


EXPERTS = 4
STEPS = 2
CAP = 24
SPAN = EXPERTS * CAP
EIGHTHS = (3, 3, 2)
MIB = 1 << 20
epsilon = 1e-05


HBM = pl.BlockSpec(memory_space=pl.ANY)
WHOLE = pl.BlockSpec(memory_space=pltpu.VMEM)


def in_hbm(w):
    return pltpu.with_memory_space_constraint(w, pltpu.HBM)


def in_vmem(w):
    return pltpu.with_memory_space_constraint(w, pltpu.VMEM)


def limit(n):
    return pltpu.CompilerParams(vmem_limit_bytes=int(n))


def tile_of(width, most):
    return next(t for t in (most, 256, 128, width) if width % t == 0)


def call(kernel, *args, keep=(), after=(), **kwargs):
    count, extra = len(args), len(keep) + len(after)
    body = lambda *refs: kernel(*refs[:count], *refs[count + extra:])
    specs = kwargs.pop("in_specs", [WHOLE] * count)
    return pl.pallas_call(body, in_specs=list(specs) + [WHOLE] * len(keep) + [HBM] * len(after), **kwargs)(*args, *map(in_vmem, keep), *after)


def own_expert():
    return lax.axis_index("expert") // (lax.axis_size("expert") // EXPERTS)


def slot_table(chosen, first, second):
    tokens = chosen.shape[0]
    own = own_expert()
    a, b = chosen[:, 0:1] ^ own, chosen[:, 1:2] ^ own
    lane = lax.broadcasted_iota(jnp.int32, (tokens, 128), 1)
    hit = ((a == lane) | (b == lane)).astype(jnp.float32)
    earlier = lax.broadcasted_iota(jnp.int32, (tokens, tokens), 1) < lax.broadcasted_iota(jnp.int32, (tokens, tokens), 0)
    before = jnp.dot(earlier.astype(jnp.float32), hit, preferred_element_type=jnp.float32).astype(jnp.int32)
    column = lax.broadcasted_iota(jnp.int32, (tokens, SPAN), 1)
    table = jnp.zeros((tokens, SPAN), jnp.float32)
    for k in range(EXPERTS):
        share = jnp.where(a == k, first, jnp.where(b == k, second, 0.0))
        table = jnp.where(column == k * CAP + before[:, k:k + 1], share, table)
    return table


def route_kernel(t, parts, arrives):
    def kernel(*refs):
        x_refs, refs = refs[:parts], refs[parts:]
        arriving_ref, refs = (refs[0], refs[1:]) if arrives else (None, refs)
        scale_ref, chosen_ref, normed_ref, *refs = refs
        x = jnp.concatenate([ref[...] for ref in x_refs], 1) if parts > 1 else x_refs[0][...]
        if arrives:
            piece_refs, x_ref = refs[:-1], refs[-1]
            x = jnp.where(lax.axis_index("section") == 0, arriving_ref[...], x)
            x_ref[...] = x
        else:
            piece_refs = refs
        x = x.astype(jnp.float32)
        mean = jnp.mean(x * x, -1, keepdims=True)
        normed = (x * lax.rsqrt(mean + epsilon) * scale_ref[...]).astype(jnp.bfloat16)
        normed_ref[...] = normed
        table = slot_table(chosen_ref[t], 1.0, 1.0).astype(jnp.bfloat16)
        rows = lax.dot_general(table, normed, (((0,), (0,)), ((), ())), preferred_element_type=jnp.float32).astype(jnp.bfloat16)
        for k, ref in enumerate(piece_refs):
            ref[...] = rows[k * CAP:(k + 1) * CAP]

    return kernel


def route(t, x_parts, arriving, scale, chosen):
    tokens, width = x_parts[0].shape[0], scale.shape[1]
    whole = jax.ShapeDtypeStruct((tokens, width), jnp.bfloat16)
    piece = jax.ShapeDtypeStruct((CAP, width), jnp.bfloat16)
    arrives = arriving is not None
    return call(
        route_kernel(t, len(x_parts), arrives),
        *x_parts, *([arriving] if arrives else []), scale, chosen,
        out_shape=[whole] + [piece] * EXPERTS + [whole] * arrives,
        compiler_params=limit(8 * MIB),
        name="route",
    )


def share_kernel(t):
    def kernel(normed_ref, router_ref, chosen_ref, table_ref):
        normed = normed_ref[...].astype(jnp.float32)
        chosen = chosen_ref[t]
        logits = [jnp.sum(normed * router_ref[e:e + 1, :], -1, keepdims=True) for e in range(EXPERTS)]
        picked = [sum(jnp.where(chosen[:, c:c + 1] == e, logits[e], 0.0) for e in range(EXPERTS)) for c in range(2)]
        first = jax.nn.sigmoid(picked[0] - picked[1])
        table_ref[...] = slot_table(chosen, first, 1.0 - first).astype(jnp.bfloat16)

    return kernel


def share_table(t, normed, router, chosen):
    return call(
        share_kernel(t),
        normed, router, chosen,
        out_shape=jax.ShapeDtypeStruct((normed.shape[0], SPAN), jnp.bfloat16),
        compiler_params=limit(4 * MIB),
        cost_estimate=pl.CostEstimate(flops=300_000_000, bytes_accessed=0, transcendentals=0),
        name="share_table",
    )


def fetch(w, rows, columns, after):
    def kernel(source_ref, target_ref):
        pltpu.sync_copy(source_ref.at[pl.ds(*rows), pl.ds(*columns)], target_ref)

    return call(
        kernel,
        in_hbm(w),
        after=after,
        in_specs=[HBM],
        out_specs=WHOLE,
        out_shape=pltpu.VMEM((rows[1], columns[1]), w.dtype),
        compiler_params=limit(MIB),
        cost_estimate=pl.CostEstimate(flops=300 * rows[1] * columns[1], bytes_accessed=4 * rows[1] * columns[1], transcendentals=0),
        name="fetch",
    )


def gather_kernel(*refs):
    *piece_refs, low_ref, high_ref = refs
    half = low_ref.shape[1]
    for i, ref in enumerate(piece_refs):
        low_ref[i * CAP:(i + 1) * CAP, :] = ref[:, :half]
        high_ref[i * CAP:(i + 1) * CAP, :] = ref[:, half:]


def gather(pieces):
    return call(
        gather_kernel,
        *pieces,
        out_shape=[jax.ShapeDtypeStruct((len(pieces) * CAP, pieces[0].shape[1] // 2), jnp.bfloat16)] * 2,
        compiler_params=limit(MIB),
        name="gather",
    )


def expand_kernel(low_ref, high_ref, held_ref, gate_ref, up_ref, hidden_ref, ring_ref, sems, gate_sum_ref, up_sum_ref):
    half = held_ref.shape[0]
    tile = ring_ref.shape[2]
    count = hidden_ref.shape[1] // tile
    streams = ((up_ref, 0), (up_ref, 1), (gate_ref, 1))

    def copy(n, j):
        ref, k = streams[j]
        source = ref.at[pl.ds(k * half, half), pl.ds(pl.multiple_of(n * tile, tile), tile)]
        return pltpu.make_async_copy(source, ring_ref.at[j], sems.at[j])

    for j in range(len(streams)):
        copy(0, j).start()

    def step(n, carry):
        def product(rows_ref, j):
            copy(n, j).wait()
            return jnp.dot(rows_ref[...], ring_ref[j], preferred_element_type=jnp.float32)

        def refill(j):
            @pl.when(n + 1 < count)
            def _():
                copy(n + 1, j).start()

        columns = pl.ds(pl.multiple_of(n * tile, tile), tile)
        gate_sum_ref[...] = jnp.dot(low_ref[...], held_ref[:, columns], preferred_element_type=jnp.float32)
        up_sum_ref[...] = product(low_ref, 0)
        refill(0)
        up_sum_ref[...] += product(high_ref, 1)
        refill(1)
        gate = gate_sum_ref[...] + product(high_ref, 2)
        refill(2)
        hidden_ref[:, columns] = (gate * jax.nn.sigmoid(gate) * up_sum_ref[...]).astype(jnp.bfloat16)
        return carry

    lax.fori_loop(0, count, step, 0)


def expand(low, high, held, gate_w, up_w):
    depth, units = up_w.shape
    tile = tile_of(units, 512)
    total = low.shape[0]
    half = held.shape[0]
    return call(
        expand_kernel,
        low, high, in_vmem(held), in_hbm(gate_w), in_hbm(up_w),
        in_specs=[WHOLE] * 3 + [HBM] * 2,
        out_shape=jax.ShapeDtypeStruct((total, units), jnp.bfloat16),
        scratch_shapes=[pltpu.VMEM((3, half, tile), jnp.bfloat16), pltpu.SemaphoreType.DMA((3,)), pltpu.VMEM((total, tile), jnp.float32), pltpu.VMEM((total, tile), jnp.float32)],
        compiler_params=limit(6 * half * tile + 12 * total * tile + 5 * total * half),
        cost_estimate=pl.CostEstimate(flops=4 * total * depth * units, bytes_accessed=2 * depth * units, transcendentals=total * units),
        name="expand",
    )


def contract_kernel(hidden_ref, down_ref, own_ref, *other):
    width = down_ref.shape[1]
    tile = tile_of(width, 512)
    for start in range(0, width, tile):
        columns = slice(start, start + tile)
        out = jnp.dot(hidden_ref[...], down_ref[:, columns], preferred_element_type=jnp.float32)
        own_ref[:, columns] = out[:SPAN]
        for m, ref in enumerate(other):
            ref[:, columns] = out[(m + 1) * SPAN:(m + 2) * SPAN].astype(jnp.bfloat16)


def contract(hidden, held, keep, after):
    total, units = hidden.shape
    width = held.shape[1]
    tile = tile_of(width, 512)
    others = total // SPAN - 1
    return call(
        contract_kernel,
        hidden, in_vmem(held),
        keep=keep,
        after=after,
        out_shape=[jax.ShapeDtypeStruct((SPAN, width), jnp.float32)] + [jax.ShapeDtypeStruct((SPAN, width), jnp.bfloat16)] * others,
        compiler_params=limit(16 * total * tile + 2 * MIB),
        cost_estimate=pl.CostEstimate(flops=2 * total * width * units, bytes_accessed=2 * width * units, transcendentals=0),
        name="contract",
    )


def merge_kernel(*refs):
    own_ref, other_refs, piece_refs = refs[0], refs[1:-EXPERTS], refs[-EXPERTS:]
    total = own_ref[...]
    for ref in other_refs:
        total = total + ref[...].astype(jnp.float32)
    total = total.astype(jnp.bfloat16)
    for k, ref in enumerate(piece_refs):
        ref[...] = total[k * CAP:(k + 1) * CAP]


def merge(own, others):
    return call(
        merge_kernel,
        own, *others,
        out_shape=[jax.ShapeDtypeStruct((CAP, own.shape[1]), jnp.bfloat16)] * EXPERTS,
        compiler_params=limit(4 * MIB),
        name="merge",
    )


def combine_kernel(start):
    def kernel(table_ref, x_ref, *refs):
        *piece_refs, out_ref = refs
        rows = jnp.concatenate([ref[...] for ref in piece_refs], 0)
        mixture = jnp.dot(table_ref[...], rows, preferred_element_type=jnp.float32)
        x = x_ref[:, start:start + out_ref.shape[1]].astype(jnp.float32)
        out_ref[...] = (x + mixture).astype(jnp.bfloat16)

    return kernel


def combine(table, x, pieces, start):
    return call(
        combine_kernel(start),
        table, x, *pieces,
        out_shape=jax.ShapeDtypeStruct((x.shape[0], pieces[0].shape[1]), jnp.bfloat16),
        compiler_params=limit(4 * MIB),
        name="combine",
    )


def over_experts(v, k):
    group = lax.axis_size("expert") // EXPERTS
    return lax.ppermute(v, "expert", [(e * group + j, (e ^ k) * group + j) for e in range(EXPERTS) for j in range(group)]) if k else v


def over_group(v, m):
    group = lax.axis_size("expert") // EXPERTS
    return lax.ppermute(v, "expert", [(e * group + j, e * group + (j + m) % group) for e in range(EXPERTS) for j in range(group)])


def over_sections(v):
    n = lax.axis_size("section")
    return lax.ppermute(v, "section", [(i, (i + 1) % n) for i in range(n)])


def moe_layer(t, x_parts, arriving, chosen, scale, router, gate_w, up_w, down_w, held):
    group = lax.axis_size("expert") // EXPERTS
    width = down_w.shape[1]
    normed, *routed = route(t, x_parts, arriving, scale, chosen)
    x = x_parts[0] if arriving is None else routed.pop()
    mine = [None] * EXPERTS
    for k in (3, 2, 1, 0):
        mine[k] = over_experts(routed[k], k)
    pieces = list(mine)
    for m in range(1, group):
        for piece in mine:
            pieces.append(over_group(piece, m))
    table = share_table(t, normed, router, chosen)
    widths = [width * e // 8 for e in EIGHTHS]
    starts = [sum(widths[:c]) for c in range(len(widths))]
    if not held:
        half = gate_w.shape[0] // 2
        down = []
        for span in zip(starts, widths):
            down.append(fetch(down_w, (0, down_w.shape[0]), span, [routed[0]]))
        gate = fetch(gate_w, (0, half), (0, gate_w.shape[1]), [routed[0]])
        held = gate, *down
    hidden = expand(*gather(pieces), held[0], gate_w, up_w)
    outs = []
    after = []
    for c, start in enumerate(starts):
        own, *others = contract(hidden, held[1 + c], [h for i, h in enumerate(held) if i != 1 + c], after)
        after = [own]
        others = [over_group(other, -m) for m, other in enumerate(others, 1)]
        back = list(merge(own, others))
        for k in (3, 2, 1):
            back[k] = over_experts(back[k], k)
        out = combine(table, x, back, start)
        outs.append(over_sections(out))
    return outs, held


def shards(pending, arriving, assignment, scale, router, gate_w, up_w, down_w):
    chosen = assignment[0]
    columns = router[0].T
    parts = [pending[0]]
    records = []
    held = ()
    for t in range(STEPS):
        parts, held = moe_layer(t, parts, arriving[t - 1] if t else None, chosen, scale, columns, gate_w[0], up_w[0], down_w[0], held)
        records.append(jnp.concatenate(parts, -1))
    return jnp.stack(records)[:, None]


def solution(mesh):
    return jax.shard_map(
        shards,
        mesh=mesh,
        in_specs=(
            P("section", "expert", None),
            P(None, "expert", None),
            P("section", None, "expert", None),
            P("section", None),
            P("section", None, None),
            P("section", None, "expert"),
            P("section", None, "expert"),
            P("section", "expert", None),
        ),
        out_specs=P(None, "section", "expert", None),
        check_vma=False,
    )
```

```python
import jax
import jax.numpy as jnp
from jax import lax
from jax.experimental import pallas as pl
from jax.experimental.pallas import tpu as pltpu
from jax.sharding import PartitionSpec as P


EXPERTS = 4
STEPS = 2
CAP = 24
SPAN = EXPERTS * CAP
EIGHTHS = (3, 3, 2)
TURNS = (1, 3, 2)
RETURNS = (3, 2, 1)
MIB = 1 << 20
epsilon = 1e-05


HBM = pl.BlockSpec(memory_space=pl.ANY)
WHOLE = pl.BlockSpec(memory_space=pltpu.VMEM)


def in_hbm(w):
    return pltpu.with_memory_space_constraint(w, pltpu.HBM)


def in_vmem(w):
    return pltpu.with_memory_space_constraint(w, pltpu.VMEM)


def limit(n):
    return pltpu.CompilerParams(vmem_limit_bytes=int(n))


def tile_of(width, most):
    return next(t for t in (most, 256, 128, width) if width % t == 0)


def call(kernel, *args, keep=(), after=(), **kwargs):
    count, extra = len(args), len(keep) + len(after)
    body = lambda *refs: kernel(*refs[:count], *refs[count + extra:])
    specs = kwargs.pop("in_specs", [WHOLE] * count)
    return pl.pallas_call(body, in_specs=list(specs) + [WHOLE] * len(keep) + [HBM] * len(after), **kwargs)(*args, *map(in_vmem, keep), *after)


def own_expert():
    return lax.axis_index("expert") // (lax.axis_size("expert") // EXPERTS)


def slot_table(chosen, first, second):
    tokens = chosen.shape[0]
    own = own_expert()
    a, b = chosen[:, 0:1] ^ own, chosen[:, 1:2] ^ own
    lane = lax.broadcasted_iota(jnp.int32, (tokens, 128), 1)
    hit = ((a == lane) | (b == lane)).astype(jnp.float32)
    earlier = lax.broadcasted_iota(jnp.int32, (tokens, tokens), 1) < lax.broadcasted_iota(jnp.int32, (tokens, tokens), 0)
    before = jnp.dot(earlier.astype(jnp.float32), hit, preferred_element_type=jnp.float32).astype(jnp.int32)
    column = lax.broadcasted_iota(jnp.int32, (tokens, SPAN), 1)
    table = jnp.zeros((tokens, SPAN), jnp.float32)
    for k in range(EXPERTS):
        share = jnp.where(a == k, first, jnp.where(b == k, second, 0.0))
        table = jnp.where(column == k * CAP + before[:, k:k + 1], share, table)
    return table


def route_kernel(t, parts, arrives):
    def kernel(*refs):
        x_refs, refs = refs[:parts], refs[parts:]
        arriving_ref, refs = (refs[0], refs[1:]) if arrives else (None, refs)
        scale_ref, chosen_ref, normed_ref, *refs = refs
        x = jnp.concatenate([ref[...] for ref in x_refs], 1) if parts > 1 else x_refs[0][...]
        if arrives:
            piece_refs, x_ref = refs[:-1], refs[-1]
            x = jnp.where(lax.axis_index("section") == 0, arriving_ref[...], x)
            x_ref[...] = x
        else:
            piece_refs = refs
        x = x.astype(jnp.float32)
        mean = jnp.mean(x * x, -1, keepdims=True)
        normed = (x * lax.rsqrt(mean + epsilon) * scale_ref[...]).astype(jnp.bfloat16)
        normed_ref[...] = normed
        table = slot_table(chosen_ref[t], 1.0, 1.0).astype(jnp.bfloat16)
        rows = lax.dot_general(table, normed, (((0,), (0,)), ((), ())), preferred_element_type=jnp.float32).astype(jnp.bfloat16)
        for k, ref in enumerate(piece_refs):
            ref[...] = rows[k * CAP:(k + 1) * CAP]

    return kernel


def route(t, x_parts, arriving, scale, chosen):
    tokens, width = x_parts[0].shape[0], scale.shape[1]
    whole = jax.ShapeDtypeStruct((tokens, width), jnp.bfloat16)
    piece = jax.ShapeDtypeStruct((CAP, width), jnp.bfloat16)
    arrives = arriving is not None
    return call(
        route_kernel(t, len(x_parts), arrives),
        *x_parts, *([arriving] if arrives else []), scale, chosen,
        out_shape=[whole] + [piece] * EXPERTS + [whole] * arrives,
        compiler_params=limit(8 * MIB),
        name="route",
    )


def share_kernel(t):
    def kernel(normed_ref, router_ref, chosen_ref, table_ref):
        normed = normed_ref[...].astype(jnp.float32)
        chosen = chosen_ref[t]
        logits = [jnp.sum(normed * router_ref[e:e + 1, :], -1, keepdims=True) for e in range(EXPERTS)]
        picked = [sum(jnp.where(chosen[:, c:c + 1] == e, logits[e], 0.0) for e in range(EXPERTS)) for c in range(2)]
        first = jax.nn.sigmoid(picked[0] - picked[1])
        table_ref[...] = slot_table(chosen, first, 1.0 - first).astype(jnp.bfloat16)

    return kernel


def share_table(t, normed, router, chosen):
    return call(
        share_kernel(t),
        normed, router, chosen,
        out_shape=jax.ShapeDtypeStruct((normed.shape[0], SPAN), jnp.bfloat16),
        compiler_params=limit(4 * MIB),
        cost_estimate=pl.CostEstimate(flops=300_000_000, bytes_accessed=0, transcendentals=0),
        name="share_table",
    )


def fetch(w, rows, columns, after):
    def kernel(source_ref, target_ref):
        pltpu.sync_copy(source_ref.at[pl.ds(*rows), pl.ds(*columns)], target_ref)

    return call(
        kernel,
        in_hbm(w),
        after=after,
        in_specs=[HBM],
        out_specs=WHOLE,
        out_shape=pltpu.VMEM((rows[1], columns[1]), w.dtype),
        compiler_params=limit(MIB),
        cost_estimate=pl.CostEstimate(flops=300 * rows[1] * columns[1], bytes_accessed=4 * rows[1] * columns[1], transcendentals=0),
        name="fetch",
    )


def gather_kernel(*refs):
    *piece_refs, low_ref, high_ref = refs
    half = low_ref.shape[1]
    for i, ref in enumerate(piece_refs):
        low_ref[i * CAP:(i + 1) * CAP, :] = ref[:, :half]
        high_ref[i * CAP:(i + 1) * CAP, :] = ref[:, half:]


def gather(pieces):
    return call(
        gather_kernel,
        *pieces,
        out_shape=[jax.ShapeDtypeStruct((len(pieces) * CAP, pieces[0].shape[1] // 2), jnp.bfloat16)] * 2,
        compiler_params=limit(MIB),
        name="gather",
    )


def expand_kernel(low_ref, high_ref, held_ref, gate_ref, up_ref, hidden_ref, ring_ref, sems, gate_sum_ref, up_sum_ref):
    half = held_ref.shape[0]
    tile = ring_ref.shape[2]
    count = hidden_ref.shape[1] // tile
    streams = ((up_ref, 0), (up_ref, 1), (gate_ref, 1))

    def copy(n, j):
        ref, k = streams[j]
        source = ref.at[pl.ds(k * half, half), pl.ds(pl.multiple_of(n * tile, tile), tile)]
        return pltpu.make_async_copy(source, ring_ref.at[j], sems.at[j])

    for j in range(len(streams)):
        copy(0, j).start()

    def step(n, carry):
        def product(rows_ref, j):
            copy(n, j).wait()
            return jnp.dot(rows_ref[...], ring_ref[j], preferred_element_type=jnp.float32)

        def refill(j):
            @pl.when(n + 1 < count)
            def _():
                copy(n + 1, j).start()

        columns = pl.ds(pl.multiple_of(n * tile, tile), tile)
        gate_sum_ref[...] = jnp.dot(low_ref[...], held_ref[:, columns], preferred_element_type=jnp.float32)
        up_sum_ref[...] = product(low_ref, 0)
        refill(0)
        up_sum_ref[...] += product(high_ref, 1)
        refill(1)
        gate = gate_sum_ref[...] + product(high_ref, 2)
        refill(2)
        hidden_ref[:, columns] = (gate * jax.nn.sigmoid(gate) * up_sum_ref[...]).astype(jnp.bfloat16)
        return carry

    lax.fori_loop(0, count, step, 0)


def expand(low, high, held, gate_w, up_w):
    depth, units = up_w.shape
    tile = tile_of(units, 512)
    total = low.shape[0]
    half = held.shape[0]
    return call(
        expand_kernel,
        low, high, in_vmem(held), in_hbm(gate_w), in_hbm(up_w),
        in_specs=[WHOLE] * 3 + [HBM] * 2,
        out_shape=jax.ShapeDtypeStruct((total, units), jnp.bfloat16),
        scratch_shapes=[pltpu.VMEM((3, half, tile), jnp.bfloat16), pltpu.SemaphoreType.DMA((3,)), pltpu.VMEM((total, tile), jnp.float32), pltpu.VMEM((total, tile), jnp.float32)],
        compiler_params=limit(6 * half * tile + 12 * total * tile + 5 * total * half),
        cost_estimate=pl.CostEstimate(flops=4 * total * depth * units, bytes_accessed=2 * depth * units, transcendentals=total * units),
        name="expand",
    )


def contract_kernel(hidden_ref, down_ref, own_ref, *other):
    width = down_ref.shape[1]
    tile = tile_of(width, 512)
    for start in range(0, width, tile):
        columns = slice(start, start + tile)
        out = jnp.dot(hidden_ref[...], down_ref[:, columns], preferred_element_type=jnp.float32)
        own_ref[:, columns] = out[:SPAN]
        for m, ref in enumerate(other):
            ref[:, columns] = out[(m + 1) * SPAN:(m + 2) * SPAN].astype(jnp.bfloat16)


def contract(hidden, held, keep, after):
    total, units = hidden.shape
    width = held.shape[1]
    tile = tile_of(width, 512)
    others = total // SPAN - 1
    return call(
        contract_kernel,
        hidden, in_vmem(held),
        keep=keep,
        after=after,
        out_shape=[jax.ShapeDtypeStruct((SPAN, width), jnp.float32)] + [jax.ShapeDtypeStruct((SPAN, width), jnp.bfloat16)] * others,
        compiler_params=limit(16 * total * tile + 2 * MIB),
        cost_estimate=pl.CostEstimate(flops=2 * total * width * units, bytes_accessed=2 * width * units, transcendentals=0),
        name="contract",
    )


def merge_kernel(*refs):
    own_ref, other_refs, piece_refs = refs[0], refs[1:-EXPERTS], refs[-EXPERTS:]
    total = own_ref[...]
    for ref in other_refs:
        total = total + ref[...].astype(jnp.float32)
    total = total.astype(jnp.bfloat16)
    for k, ref in enumerate(piece_refs):
        ref[...] = total[k * CAP:(k + 1) * CAP]


def merge(own, others):
    return call(
        merge_kernel,
        own, *others,
        out_shape=[jax.ShapeDtypeStruct((CAP, own.shape[1]), jnp.bfloat16)] * EXPERTS,
        compiler_params=limit(4 * MIB),
        name="merge",
    )


def combine_kernel(start):
    def kernel(table_ref, x_ref, *refs):
        *piece_refs, out_ref = refs
        rows = jnp.concatenate([ref[...] for ref in piece_refs], 0)
        mixture = jnp.dot(table_ref[...], rows, preferred_element_type=jnp.float32)
        x = x_ref[:, start:start + out_ref.shape[1]].astype(jnp.float32)
        out_ref[...] = (x + mixture).astype(jnp.bfloat16)

    return kernel


def combine(table, x, pieces, start):
    return call(
        combine_kernel(start),
        table, x, *pieces,
        out_shape=jax.ShapeDtypeStruct((x.shape[0], pieces[0].shape[1]), jnp.bfloat16),
        compiler_params=limit(4 * MIB),
        name="combine",
    )


def over_experts(v, k):
    group = lax.axis_size("expert") // EXPERTS
    return lax.ppermute(v, "expert", [(e * group + j, (e ^ k) * group + j) for e in range(EXPERTS) for j in range(group)]) if k else v


def over_group(v, m):
    group = lax.axis_size("expert") // EXPERTS
    return lax.ppermute(v, "expert", [(e * group + j, e * group + (j + m) % group) for e in range(EXPERTS) for j in range(group)])


def over_sections(v):
    n = lax.axis_size("section")
    return lax.ppermute(v, "section", [(i, (i + 1) % n) for i in range(n)])


def moe_layer(t, x_parts, arriving, chosen, scale, router, gate_w, up_w, down_w, held):
    group = lax.axis_size("expert") // EXPERTS
    width = down_w.shape[1]
    normed, *routed = route(t, x_parts, arriving, scale, chosen)
    x = x_parts[0] if arriving is None else routed.pop()
    mine = [None] * EXPERTS
    for k in (*TURNS, 0):
        mine[k] = over_experts(routed[k], k)
    pieces = list(mine)
    for m in range(1, group):
        for piece in mine:
            pieces.append(over_group(piece, m))
    table = share_table(t, normed, router, chosen)
    widths = [width * e // 8 for e in EIGHTHS]
    starts = [sum(widths[:c]) for c in range(len(widths))]
    if not held:
        half = gate_w.shape[0] // 2
        down = []
        for span in zip(starts, widths):
            down.append(fetch(down_w, (0, down_w.shape[0]), span, [routed[0]]))
        gate = fetch(gate_w, (0, half), (0, gate_w.shape[1]), [routed[0]])
        held = gate, *down
    hidden = expand(*gather(pieces), held[0], gate_w, up_w)
    outs = []
    after = []
    for c, start in enumerate(starts):
        own, *others = contract(hidden, held[1 + c], [h for i, h in enumerate(held) if i != 1 + c], after)
        after = [own]
        others = [over_group(other, -m) for m, other in enumerate(others, 1)]
        back = list(merge(own, others))
        for k in RETURNS:
            back[k] = over_experts(back[k], k)
        out = combine(table, x, back, start)
        outs.append(over_sections(out))
    return outs, held


def shards(pending, arriving, assignment, scale, router, gate_w, up_w, down_w):
    chosen = assignment[0]
    columns = router[0].T
    parts = [pending[0]]
    records = []
    held = ()
    for t in range(STEPS):
        parts, held = moe_layer(t, parts, arriving[t - 1] if t else None, chosen, scale, columns, gate_w[0], up_w[0], down_w[0], held)
        records.append(jnp.concatenate(parts, -1))
    return jnp.stack(records)[:, None]


def solution(mesh):
    return jax.shard_map(
        shards,
        mesh=mesh,
        in_specs=(
            P("section", "expert", None),
            P(None, "expert", None),
            P("section", None, "expert", None),
            P("section", None),
            P("section", None, None),
            P("section", None, "expert"),
            P("section", None, "expert"),
            P("section", "expert", None),
        ),
        out_specs=P(None, "section", "expert", None),
        check_vma=False,
    )
```
